32 devices in a mesh: arcs: 2 (over x), trow: 4 (over y, core), tcol: 4 (over z).
Axes of the slice: x: 2, y: 2, z: 4, core: 2. Of those that a mesh axis runs over, the one named last changes fastest.
Arguments:
- design: bfloat16 [1024, 12288], P(('arcs', 'tcol'), 'trow'), may hold values from -6 to 6
- observed: float32 [1024], P(('arcs', 'tcol')), may hold values from -6 to 6
- arc_counts: int32 [32], P(('arcs', 'tcol')), may hold values from 2 to 32
- arc_weight: float32 [32], P(('arcs', 'tcol')), may hold values from 0.3 to 3
Outputs:
- gram: float32 [12288, 12288], P('trow', ('arcs', 'tcol'))
- rhs: float32 [12288], P('trow')
The draws below stay inside these ranges and needn't reach their ends.
Inputs may be any that keep to these rules, and one draw needn't show every extreme that they name: `arc_counts`: each arc has at least two valid observations.
All inputs are finite; a program needn't handle non-finite values.
Results may differ from the reference program's by a relative error of at most 0.0055.
Values may be sent and summed in bfloat16 or wider, within the bound.
A program may use at most 192 MiB of HBM per device.

```python
import math
import jax
import jax.numpy as jnp
from jax import lax

K = 12288
ARC_LEN = 32
OBS = 1024
ARCS = 32


def plant(values, key, least, largest):
    index_at = [jax.random.randint(jax.random.fold_in(key, axis), (), 0, length) for axis, length in enumerate(values.shape)]
    longest = values.shape.index(max(values.shape))
    beside = index_at[:longest] + [(index_at[longest] + 1) % values.shape[longest]] + index_at[longest + 1:]
    return values.at[tuple(index_at)].set(least).at[tuple(beside)].set(largest)


def levels(own_key, extent, shards, least, largest):
    level = 1.0
    for position, blocks in shards:
        steps = jax.random.uniform(jax.random.fold_in(jax.random.fold_in(own_key, 6), position), (blocks,), jnp.float32, least / len(shards), largest / len(shards))
        level = level * jnp.repeat(jnp.exp(steps), extent[position] // blocks).reshape((-1,) + (1,) * (len(extent) - 1 - position))
    return level


def normal_values(rng, extent, spread, limit, pieces=(), held_as=jnp.bfloat16):
    level = levels(rng, extent, pieces, -0.22, 0.18) if pieces else 1.0
    entries = jax.random.normal(rng, extent, jnp.float32) * spread * level
    return jnp.minimum(jnp.maximum(entries, -limit), limit).astype(held_as)


def setup_inputs(seed: int = 0) -> dict:
    key_list = jax.random.split(jax.random.key(seed), 5)
    return {
        "design": normal_values(key_list[0], (OBS, K), 1.0, 6.0, ((0, 8), (1, 4))),
        "observed": normal_values(key_list[1], (OBS,), 1.0, 6.0, ((0, 8),), jnp.float32),
        "arc_counts": plant(jax.random.randint(key_list[2], (ARCS,), 2, ARC_LEN + 1), jax.random.fold_in(key_list[2], 1), 2, ARC_LEN).astype(jnp.int32),
        "arc_weight": jnp.clip(jnp.exp(math.log(3.0) - 2.3025851 * jax.random.uniform(key_list[3], (ARCS,), jnp.float32) ** levels(key_list[3], (ARCS,), ((0, 8),), -0.2, 0.2)), 0.3, 3.0),
    }


def reference(design, observed, arc_counts, arc_weight):
    obs_count, col_width = design.shape
    arc_total = arc_counts.shape[0]
    arc_len = obs_count // arc_total
    slot_index = lax.broadcasted_iota(jnp.int32, (arc_total, arc_len), 1)
    valid_mask = (slot_index < arc_counts[:, None]).astype(jnp.float32)
    counts_float = arc_counts.astype(jnp.float32)
    factor = valid_mask * jnp.sqrt(arc_weight)[:, None]
    blocks = design.reshape(arc_total, arc_len, col_width).astype(jnp.float32)
    column_mean = lax.optimization_barrier(jnp.sum(valid_mask[:, :, None] * blocks, axis=1)) / counts_float[:, None]
    centered = (factor[:, :, None] * (blocks - column_mean[:, None, :])).reshape(obs_count, col_width).astype(jnp.bfloat16)
    series = observed.reshape(arc_total, arc_len)
    series_mean = lax.optimization_barrier(jnp.sum(valid_mask * series, axis=1)) / counts_float
    weighted = (factor * (series - series_mean[:, None])).reshape(obs_count)
    widened = centered.astype(jnp.float32)
    gram = jnp.dot(widened.T, widened, precision=lax.Precision.HIGHEST, preferred_element_type=jnp.float32) * (1.0 / obs_count)
    rhs = jnp.dot(weighted, widened, precision=lax.Precision.HIGHEST) * obs_count ** (-0.5)
    return (gram, rhs)
```

```python
import functools
import jax
import jax.numpy as jnp
from jax import lax
from jax.experimental import pallas as pl
from jax.experimental.pallas import tpu as pltpu
from jax.sharding import PartitionSpec as P

MESH = pl.DeviceIdType.MESH
CHUNKS = 6


def fold_with(right, piece):
    return lax.dot_general(
        piece, right, (((0,), (0,)), ((), ())), preferred_element_type=jnp.float32
    )


def centre(design, observed, arc_counts, arc_weight):
    row_count, col_width = design.shape
    arc_total = arc_counts.shape[0]
    arc_len = row_count // arc_total
    slot_index = lax.broadcasted_iota(jnp.int32, (arc_total, arc_len), 1)
    valid_mask = (slot_index < arc_counts[:, None]).astype(jnp.float32)
    counts_float = arc_counts.astype(jnp.float32)
    factor = valid_mask * jnp.sqrt(arc_weight)[:, None]
    blocks = design.reshape(arc_total, arc_len, col_width).astype(jnp.float32)
    column_mean = jnp.sum(valid_mask[:, :, None] * blocks, axis=1) / counts_float[:, None]
    centered = (
        (factor[:, :, None] * (blocks - column_mean[:, None, :]))
        .reshape(row_count, col_width)
        .astype(jnp.bfloat16)
    )
    series = observed.reshape(arc_total, arc_len)
    series_mean = jnp.sum(valid_mask * series, axis=1) / counts_float
    weighted = (factor * (series - series_mean[:, None])).reshape(row_count)
    return centered, weighted


def general(design, observed, arc_counts, arc_weight):
    centered, weighted = centre(design, observed, arc_counts, arc_weight)
    row_count = design.shape[0]
    arc_devices = lax.axis_size("arcs")
    tcol_devices = lax.axis_size("tcol")
    obs_total = row_count * arc_devices * tcol_devices
    rhs_part = jnp.dot(weighted, centered.astype(jnp.float32), precision=lax.Precision.HIGHEST)
    rhs = lax.psum(rhs_part, ("arcs", "tcol")) * obs_total ** (-0.5)
    every_coef = lax.all_gather(centered, "trow", axis=1, tiled=True)
    full_width = every_coef.shape[1]
    narrow = full_width // (arc_devices * tcol_devices)
    shaped = every_coef.reshape(row_count, arc_devices * tcol_devices, narrow)
    moved = lax.all_to_all(shaped, ("arcs", "tcol"), split_axis=1, concat_axis=0, tiled=True)
    right = moved.reshape(row_count * arc_devices * tcol_devices, narrow)
    tile = fold_with(right, lax.all_gather(centered, ("arcs", "tcol"), axis=0, tiled=True))
    return (tile * (1.0 / obs_total), rhs)


OWN_X, OWN_UP, OWN_DOWN, TWO_UP, TWO_DOWN, THREE_UP, THREE_DOWN, PAIR_X, TWO_X, REST_X, PAIR_Z = range(11)


def kernel(cent, wown, gram, rhs, rows, right, wall, ssem, rsem, osem, qsem, rrsem, wssem, wrsem):
    n, _, depth, w = cent.shape
    x, t, z = lax.axis_index("arcs"), lax.axis_index("trow"), lax.axis_index("tcol")
    y, core = t // 2, t % 2
    me = x * 4 + z
    other = (1 - x) * 4
    obs_total = 8 * depth
    hz = z % 2
    pair = z + 1 - 2 * hz
    two = (z + 2) % 4
    rest = 3 - z
    xn = (1 - x, t, z)
    up = (x, t, jnp.minimum(z + 1, 3))
    down = (x, t, jnp.maximum(z - 1, 0))
    mate = (x, t, pair)
    partner = (x, t + 1 - 2 * core, z)
    yn = (x, (1 - y) * 2 + core, z)
    lead = core == z // 2
    home = y == x
    is_o = jnp.logical_and(lead, home)
    is_q = jnp.logical_and(lead, jnp.logical_not(home))
    not_lead = jnp.logical_not(lead)
    has_up, has_down = z < 3, z > 0
    inner = jnp.logical_and(has_up, has_down)
    outer = jnp.logical_not(inner)
    low, high = z < 2, z >= 2
    both = jnp.logical_and

    barrier = pltpu.get_barrier_semaphore()
    peers = []
    for dx in range(2):
        for dz in range(4):
            if dx or dz:
                peers.append((dx * 4 + dz, ((x + dx) % 2, t, (z + dz) % 4)))
    for dev in [p for _, p in peers] + [partner, yn]:
        pl.semaphore_signal(barrier, inc=1, device_id=dev, device_id_type=MESH)
    pl.semaphore_wait(barrier, len(peers) + 2)

    def remote(src, dst, send, recv, dev):
        return pltpu.make_async_remote_copy(
            src_ref=src, dst_ref=dst, send_sem=send, recv_sem=recv, device_id=dev, device_id_type=MESH
        )

    def whole(kind, c, s, dev):
        at = rows.at[c, :, s]
        return remote(at, at, ssem.at[kind, c], rsem.at[kind, c], dev)

    def half(kind, c, s, h, dev):
        at = rows.at[c, h, s]
        return remote(at, at, ssem.at[kind, c], rsem.at[kind, c], dev)

    def own(kind, c, dev):
        return remote(cent.at[c], rows.at[c, :, me], ssem.at[kind, c], rsem.at[kind, c], dev)

    def right_pair(c, s, src):
        at = right.at[c, s]
        return (
            remote(src, at, osem.at[0, c, s], rrsem.at[c, s], partner),
            remote(src, at, osem.at[1, c, s], rrsem.at[c, s], yn),
        )

    def right_out(c, s):
        @pl.when(is_o)
        def _():
            a, b = right_pair(c, s, rows.at[c, hz, s])
            b.start()
            a.start()

    def relay_copy(c, s):
        at = right.at[c, s]
        return remote(at, at, qsem.at[c, s], rrsem.at[c, s], partner)

    def relay(c, s):
        @pl.when(is_q)
        def _():
            d = relay_copy(c, s)
            d.wait_recv()
            d.start()

    def each(body):
        def step(c, carry):
            body(c)
            return carry

        lax.fori_loop(0, n, step, 0)

    def wcopy(k, dev):
        return remote(wown, wall.at[me], wssem.at[k], wrsem.at[k], dev)

    def phase0(c):
        own(OWN_X, c, xn).start()
        pl.when(has_up)(lambda: own(OWN_UP, c, up).start())
        pl.when(has_down)(lambda: own(OWN_DOWN, c, down).start())

        @pl.when(is_o)
        def _():
            a, b = right_pair(c, me, cent.at[c, hz])
            b.start()
            a.start()

    each(phase0)
    for k, dev in peers:
        wcopy(k, dev).start()
    wall[me] = wown[...]

    def copy_own(c):
        rows[c, :, me] = cent[c]

    each(copy_own)

    def phase1(c):
        @pl.when(has_down)
        def _():
            whole(OWN_UP, c, me - 1, up).wait_recv()
            pl.when(has_up)(lambda: whole(TWO_UP, c, me - 1, up).start())

        @pl.when(has_up)
        def _():
            whole(OWN_DOWN, c, me + 1, down).wait_recv()
            pl.when(has_down)(lambda: whole(TWO_DOWN, c, me + 1, down).start())

        half(PAIR_X, c, x * 4 + pair, hz, xn).start()
        pl.when(inner)(lambda: whole(REST_X, c, x * 4 + rest, xn).start())
        right_out(c, x * 4 + pair)
        pl.when(inner)(lambda: right_out(c, x * 4 + rest))
        whole(OWN_X, c, other + z, xn).wait_recv()
        right_out(c, other + z)
        relay(c, me)

    each(phase1)

    def phase2(c):
        s = x * 4 + two

        @pl.when(low)
        def _():
            whole(TWO_DOWN, c, s, down).wait_recv()
            pl.when(z == 1)(lambda: whole(THREE_DOWN, c, s, down).start())

        @pl.when(high)
        def _():
            whole(TWO_UP, c, s, up).wait_recv()
            pl.when(z == 2)(lambda: whole(THREE_UP, c, s, up).start())

        whole(TWO_X, c, s, xn).start()
        right_out(c, s)
        half(PAIR_X, c, other + pair, hz, xn).wait_recv()
        right_out(c, other + pair)
        relay(c, x * 4 + pair)
        pl.when(inner)(lambda: relay(c, x * 4 + rest))
        relay(c, other + z)

    each(phase2)
    each(lambda c: half(PAIR_Z, c, other + z, hz, mate).start())

    def phase3(c):
        @pl.when(outer)
        def _():
            s = x * 4 + rest
            pl.when(z == 0)(lambda: whole(THREE_DOWN, c, s, down).wait_recv())
            pl.when(z == 3)(lambda: whole(THREE_UP, c, s, up).wait_recv())
            whole(REST_X, c, s, xn).start()
            right_out(c, s)

        whole(TWO_X, c, other + two, xn).wait_recv()
        right_out(c, other + two)
        relay(c, x * 4 + two)
        relay(c, other + pair)

    each(phase3)

    for k, dev in peers:
        wcopy(k, dev).wait_recv()
    wide = jnp.concatenate([wall[s] for s in range(8)], axis=1)
    hi = wide.astype(jnp.bfloat16).astype(jnp.float32)
    mid = (wide - hi).astype(jnp.bfloat16).astype(jnp.float32)
    low_part = wide - hi - mid
    pick = lax.broadcasted_iota(jnp.int32, wide.shape, 0)
    terms = jnp.where(pick == 0, hi, jnp.where(pick == 1, mid, jnp.where(pick == 2, low_part, 0.0)))
    terms = terms.astype(jnp.bfloat16)

    def tile(c1, c2):
        b = right[c2].reshape(obs_total, w)
        for h in range(2):
            a = rows[c1, h].reshape(obs_total, w)
            gram[pl.ds(pl.multiple_of(h * n * w + c1 * w, w), w), pl.ds(pl.multiple_of(c2 * w, w), w)] = fold_with(
                b, a
            ) * (1.0 / obs_total)

    def finish(c):
        relay(c, other + rest)

        @pl.when(not_lead)
        def _():
            for s in range(8):
                relay_copy(c, s).wait_recv()

        @pl.when(is_o)
        def _():
            right[c] = rows[c, hz]

        for h in range(2):
            a = rows[c, h].reshape(obs_total, w)
            part = lax.dot_general(terms, a, (((1,), (0,)), ((), ())), preferred_element_type=jnp.float32)
            rhs[pl.ds(h * n + c, 1), :] = jnp.sum(part, axis=0, keepdims=True) * obs_total ** (-0.5)

        def step(k, carry):
            tile(c, k)
            tile(k, c)
            return carry

        lax.fori_loop(0, c, step, 0)
        tile(c, c)

    def phase4(c):
        whole(REST_X, c, other + rest, xn).wait_recv()
        right_out(c, other + rest)

        @pl.when(outer)
        def _():
            s = x * 4 + rest
            relay(c, s)

        relay(c, other + two)
        half(PAIR_Z, c, other + pair, 1 - hz, mate).wait_recv()
        pl.when(c > 0)(lambda: finish(c - 1))

    each(phase4)
    finish(n - 1)

    def drain(c):
        own(OWN_X, c, xn).wait_send()
        pl.when(has_up)(lambda: own(OWN_UP, c, up).wait_send())
        pl.when(has_down)(lambda: own(OWN_DOWN, c, down).wait_send())

        @pl.when(inner)
        def _():
            whole(TWO_UP, c, me - 1, up).wait_send()
            whole(TWO_DOWN, c, me + 1, down).wait_send()

        pl.when(z == 1)(lambda: whole(THREE_DOWN, c, me, down).wait_send())
        pl.when(z == 2)(lambda: whole(THREE_UP, c, me, up).wait_send())
        half(PAIR_X, c, me, hz, xn).wait_send()
        whole(TWO_X, c, me, xn).wait_send()
        whole(REST_X, c, me, xn).wait_send()
        half(PAIR_Z, c, me, hz, mate).wait_send()

        def pieces(s, carry):
            @pl.when(is_o)
            def _():
                a, b = right_pair(c, s, rows.at[c, hz, s])
                a.wait_send()
                b.wait_send()

            pl.when(is_q)(lambda: relay_copy(c, s).wait_send())
            return carry

        lax.fori_loop(0, 8, pieces, 0)

    each(drain)
    for k, dev in peers:
        wcopy(k, dev).wait_send()


def gathered(design, observed, arc_counts, arc_weight):
    centered, weighted = centre(design, observed, arc_counts, arc_weight)
    depth, width = design.shape
    n = CHUNKS
    w = width // (2 * n)
    cent = centered.reshape(depth, 2, n, w).transpose(2, 1, 0, 3)
    wown = jnp.broadcast_to(weighted[None, :], (8, depth))
    vmem = pl.BlockSpec(memory_space=pltpu.VMEM)
    dma = pltpu.SemaphoreType.DMA
    gram, rhs = pl.pallas_call(
        kernel,
        out_shape=(
            pltpu.VMEM((width, n * w), jnp.float32) if IN_VMEM else jax.ShapeDtypeStruct((width, n * w), jnp.float32),
            jax.ShapeDtypeStruct((2 * n, w), jnp.float32),
        ),
        in_specs=[vmem, vmem],
        out_specs=(vmem, vmem),
        scratch_shapes=[
            pltpu.VMEM((n, 2, 8, depth, w), jnp.bfloat16),
            pltpu.VMEM((n, 8, depth, w), jnp.bfloat16),
            pltpu.VMEM((8, 8, depth), jnp.float32),
            dma((11, n)),
            dma((11, n)),
            dma((2, n, 8)),
            dma((n, 8)),
            dma((n, 8)),
            dma((8,)),
            dma((8,)),
        ],
        compiler_params=pltpu.CompilerParams(
            collective_id=0, has_side_effects=True, vmem_limit_bytes=VMEM_LIMIT
        ),
    )(cent, wown)
    return gram, rhs.reshape(width)


IN_VMEM = True
VMEM_LIMIT = 40 * 1024 * 1024


def solution(mesh):
    sizes = (mesh.shape["arcs"], mesh.shape["trow"], mesh.shape["tcol"])

    def local(design, observed, arc_counts, arc_weight):
        fits = sizes == (2, 4, 4) and design.shape[0] == 128 and design.shape[1] % (2 * CHUNKS * 128) == 0
        body = gathered if fits else general
        return body(design, observed, arc_counts, arc_weight)

    return jax.shard_map(
        local,
        mesh=mesh,
        in_specs=(
            P(("arcs", "tcol"), "trow"),
            P(("arcs", "tcol")),
            P(("arcs", "tcol")),
            P(("arcs", "tcol")),
        ),
        out_specs=(P("trow", ("arcs", "tcol")), P("trow")),
        check_vma=False,
    )
```

```python
import functools
import jax
import jax.numpy as jnp
from jax import lax
from jax.experimental import pallas as pl
from jax.experimental.pallas import tpu as pltpu
from jax.sharding import PartitionSpec as P

MESH = pl.DeviceIdType.MESH
CHUNKS = 6


def fold_with(right, piece):
    return lax.dot_general(
        piece, right, (((0,), (0,)), ((), ())), preferred_element_type=jnp.float32
    )


def centre(design, observed, arc_counts, arc_weight):
    row_count, col_width = design.shape
    arc_total = arc_counts.shape[0]
    arc_len = row_count // arc_total
    slot_index = lax.broadcasted_iota(jnp.int32, (arc_total, arc_len), 1)
    valid_mask = (slot_index < arc_counts[:, None]).astype(jnp.float32)
    counts_float = arc_counts.astype(jnp.float32)
    factor = valid_mask * jnp.sqrt(arc_weight)[:, None]
    blocks = design.reshape(arc_total, arc_len, col_width).astype(jnp.float32)
    column_mean = jnp.sum(valid_mask[:, :, None] * blocks, axis=1) / counts_float[:, None]
    centered = (
        (factor[:, :, None] * (blocks - column_mean[:, None, :]))
        .reshape(row_count, col_width)
        .astype(jnp.bfloat16)
    )
    series = observed.reshape(arc_total, arc_len)
    series_mean = jnp.sum(valid_mask * series, axis=1) / counts_float
    weighted = (factor * (series - series_mean[:, None])).reshape(row_count)
    return centered, weighted


def general(design, observed, arc_counts, arc_weight):
    centered, weighted = centre(design, observed, arc_counts, arc_weight)
    row_count = design.shape[0]
    arc_devices = lax.axis_size("arcs")
    tcol_devices = lax.axis_size("tcol")
    obs_total = row_count * arc_devices * tcol_devices
    rhs_part = jnp.dot(weighted, centered.astype(jnp.float32), precision=lax.Precision.HIGHEST)
    rhs = lax.psum(rhs_part, ("arcs", "tcol")) * obs_total ** (-0.5)
    every_coef = lax.all_gather(centered, "trow", axis=1, tiled=True)
    full_width = every_coef.shape[1]
    narrow = full_width // (arc_devices * tcol_devices)
    shaped = every_coef.reshape(row_count, arc_devices * tcol_devices, narrow)
    moved = lax.all_to_all(shaped, ("arcs", "tcol"), split_axis=1, concat_axis=0, tiled=True)
    right = moved.reshape(row_count * arc_devices * tcol_devices, narrow)
    tile = fold_with(right, lax.all_gather(centered, ("arcs", "tcol"), axis=0, tiled=True))
    return (tile * (1.0 / obs_total), rhs)


OWN_X, OWN_UP, OWN_DOWN, TWO_UP, TWO_DOWN, THREE_UP, THREE_DOWN, PAIR_X, TWO_X, REST_X, PAIR_Z = range(11)


def kernel(
    design, series, counts, weights, gram, rhs, rows, right, flipped, ready, wown, wall, share, scale,
    ssem, rsem, osem, qsem, rrsem, wssem, wrsem,
):
    n, _, _, depth, w = rows.shape
    arcs_here = counts.shape[0]
    arc_len = depth // arcs_here
    x, t, z = lax.axis_index("arcs"), lax.axis_index("trow"), lax.axis_index("tcol")
    y, core = t // 2, t % 2
    me = x * 4 + z
    other = (1 - x) * 4
    obs_total = 8 * depth
    hz = z % 2
    pair = z + 1 - 2 * hz
    two = (z + 2) % 4
    rest = 3 - z
    xn = (1 - x, t, z)
    up = (x, t, jnp.minimum(z + 1, 3))
    down = (x, t, jnp.maximum(z - 1, 0))
    mate = (x, t, pair)
    partner = (x, t + 1 - 2 * core, z)
    yn = (x, (1 - y) * 2 + core, z)
    lead = core == z // 2
    home = y == x
    is_o = jnp.logical_and(lead, home)
    is_q = jnp.logical_and(lead, jnp.logical_not(home))
    has_up, has_down = z < 3, z > 0
    inner = jnp.logical_and(has_up, has_down)
    outer = jnp.logical_not(inner)
    low, high = z < 2, z >= 2

    barrier = pltpu.get_barrier_semaphore()
    peers = []
    for dx in range(2):
        for dz in range(4):
            if dx or dz:
                peers.append((dx * 4 + dz, ((x + dx) % 2, t, (z + dz) % 4)))
    for dev in [p for _, p in peers] + [partner, yn]:
        pl.semaphore_signal(barrier, inc=1, device_id=dev, device_id_type=MESH)

    lane = lax.broadcasted_iota(jnp.int32, (8, depth), 1)
    arc = lane // arc_len
    count = jnp.full((8, depth), 1, jnp.int32)
    weight = jnp.zeros((8, depth), jnp.float32)
    for a in range(arcs_here):
        count = jnp.where(arc == a, counts[a], count)
        weight = jnp.where(arc == a, weights[a], weight)
    valid = (lane - arc * arc_len < count).astype(jnp.float32)
    portion = valid / count.astype(jnp.float32)
    factor = valid * jnp.sqrt(weight)
    line = jnp.broadcast_to(series[...], (8, depth))
    average = jnp.zeros((8, depth), jnp.float32)
    for a in range(arcs_here):
        total = jnp.sum(jnp.where(arc == a, valid * line, 0.0), axis=1, keepdims=True)
        average = jnp.where(arc == a, total / count.astype(jnp.float32), average)
    weighted = factor * (line - average)
    level = lax.broadcasted_iota(jnp.int32, (8, depth), 0)
    wown[...] = jnp.where(level == 0, weighted, jnp.where(level == 1, portion, factor))
    wall[me] = wown[...]
    pl.semaphore_wait(barrier, len(peers) + 2)

    def remote(src, dst, send, recv, dev):
        return pltpu.make_async_remote_copy(
            src_ref=src, dst_ref=dst, send_sem=send, recv_sem=recv, device_id=dev, device_id_type=MESH
        )

    def whole(kind, c, s, dev):
        at = rows.at[c, :, s]
        return remote(at, at, ssem.at[kind, c], rsem.at[kind, c], dev)

    def half(kind, c, s, h, dev):
        at = rows.at[c, h, s]
        return remote(at, at, ssem.at[kind, c], rsem.at[kind, c], dev)

    def mine(c, h):
        return design.at[:, pl.ds(pl.multiple_of((h * n + c) * w, w), w)]

    def own(kind, c, dev):
        for h in range(2):
            remote(mine(c, h), rows.at[c, h, me], ssem.at[kind, c], rsem.at[kind, c], dev).start()

    def right_pair(c, s, src):
        at = right.at[c, s]
        return (
            remote(src, at, osem.at[0, c, s], rrsem.at[c, s], partner),
            remote(src, at, osem.at[1, c, s], rrsem.at[c, s], yn),
        )

    def right_out(c, s):
        @pl.when(is_o)
        def _():
            a, b = right_pair(c, s, rows.at[c, hz, s])
            b.start()
            a.start()

    def relay_copy(c, s):
        at = right.at[c, s]
        return remote(at, at, qsem.at[c, s], rrsem.at[c, s], partner)

    def centre_block(block, s):
        wide = block.astype(jnp.float32).reshape(arcs_here, arc_len, w)
        part = jnp.concatenate([share[s]] * (w // 128), axis=1).reshape(arcs_here, arc_len, w)
        gain = jnp.concatenate([scale[s]] * (w // 128), axis=1).reshape(arcs_here, arc_len, w)
        mean = jnp.sum(part * wide, axis=1, keepdims=True)
        return (gain * (wide - mean)).reshape(depth, w).astype(jnp.bfloat16)

    def take(c, s):
        for h in range(2):
            flipped[c, pl.ds(h * w, w), pl.ds(pl.multiple_of(s * depth, depth), depth)] = centre_block(
                rows[c, h, s], s
            ).T

    def relay(c, s):
        @pl.when(jnp.logical_not(is_o))
        def _():
            d = relay_copy(c, s)
            d.wait_recv()
            pl.when(is_q)(d.start)
            ready[c, pl.ds(pl.multiple_of(s * depth, depth), depth), :] = centre_block(right[c, s], s)

        @pl.when(is_o)
        def _():
            ready[c, pl.ds(pl.multiple_of(s * depth, depth), depth), :] = centre_block(rows[c, hz, s], s)

    def each(body):
        def step(c, carry):
            body(c)
            return carry

        lax.fori_loop(0, n, step, 0)

    def wcopy(k, dev):
        return remote(wown, wall.at[me], wssem.at[k], wrsem.at[k], dev)

    def phase0(c):
        own(OWN_X, c, xn)
        pl.when(has_up)(lambda: own(OWN_UP, c, up))
        pl.when(has_down)(lambda: own(OWN_DOWN, c, down))

        @pl.when(is_o)
        def _():
            a, b = right_pair(c, me, mine(c, hz))
            b.start()
            a.start()

    for k, dev in peers:
        wcopy(k, dev).start()
    each(phase0)

    def copy_own(c):
        for h in range(2):
            rows[c, h, me] = design[:, pl.ds(pl.multiple_of((h * n + c) * w, w), w)]

    each(copy_own)
    for k, dev in peers:
        wcopy(k, dev).wait_recv()

    def spread(s, carry):
        columns = wall[s].T
        share[s] = jnp.broadcast_to(columns[:, 1:2], (depth, 128))
        scale[s] = jnp.broadcast_to(columns[:, 2:3], (depth, 128))
        return carry

    lax.fori_loop(0, 8, spread, 0)
    each(lambda c: take(c, me))

    def phase1(c):
        @pl.when(has_down)
        def _():
            whole(OWN_UP, c, me - 1, up).wait_recv()
            pl.when(has_up)(lambda: whole(TWO_UP, c, me - 1, up).start())

        @pl.when(has_up)
        def _():
            whole(OWN_DOWN, c, me + 1, down).wait_recv()
            pl.when(has_down)(lambda: whole(TWO_DOWN, c, me + 1, down).start())

        half(PAIR_X, c, x * 4 + pair, hz, xn).start()
        pl.when(inner)(lambda: whole(REST_X, c, x * 4 + rest, xn).start())
        right_out(c, x * 4 + pair)
        pl.when(inner)(lambda: right_out(c, x * 4 + rest))
        whole(OWN_X, c, other + z, xn).wait_recv()
        right_out(c, other + z)
        take(c, x * 4 + pair)
        pl.when(inner)(lambda: take(c, x * 4 + rest))
        take(c, other + z)
        relay(c, me)

    each(phase1)

    def phase2(c):
        s = x * 4 + two

        @pl.when(low)
        def _():
            whole(TWO_DOWN, c, s, down).wait_recv()
            pl.when(z == 1)(lambda: whole(THREE_DOWN, c, s, down).start())

        @pl.when(high)
        def _():
            whole(TWO_UP, c, s, up).wait_recv()
            pl.when(z == 2)(lambda: whole(THREE_UP, c, s, up).start())

        whole(TWO_X, c, s, xn).start()
        right_out(c, s)
        half(PAIR_X, c, other + pair, hz, xn).wait_recv()
        right_out(c, other + pair)
        take(c, s)
        relay(c, x * 4 + pair)
        pl.when(inner)(lambda: relay(c, x * 4 + rest))
        relay(c, other + z)

    each(phase2)
    each(lambda c: half(PAIR_Z, c, other + z, hz, mate).start())

    def phase3(c):
        @pl.when(outer)
        def _():
            s = x * 4 + rest
            pl.when(z == 0)(lambda: whole(THREE_DOWN, c, s, down).wait_recv())
            pl.when(z == 3)(lambda: whole(THREE_UP, c, s, up).wait_recv())
            whole(REST_X, c, s, xn).start()
            right_out(c, s)
            take(c, s)

        whole(TWO_X, c, other + two, xn).wait_recv()
        right_out(c, other + two)
        take(c, other + two)
        relay(c, x * 4 + two)
        relay(c, other + pair)

    each(phase3)

    wide = jnp.concatenate([jnp.broadcast_to(wall[s][0:1], (8, depth)) for s in range(8)], axis=1)
    hi = wide.astype(jnp.bfloat16).astype(jnp.float32)
    mid = (wide - hi).astype(jnp.bfloat16).astype(jnp.float32)
    low_part = wide - hi - mid
    pick = lax.broadcasted_iota(jnp.int32, wide.shape, 0)
    terms = jnp.where(pick == 0, hi, jnp.where(pick == 1, mid, jnp.where(pick == 2, low_part, 0.0)))
    terms = terms.astype(jnp.bfloat16)

    def tile(c1, c2):
        both_parts = lax.dot_general(
            flipped[c1], ready[c2], (((1,), (0,)), ((), ())), preferred_element_type=jnp.float32
        ) * (1.0 / obs_total)
        for h in range(2):
            gram[
                pl.ds(pl.multiple_of(h * n * w + c1 * w, w), w), pl.ds(pl.multiple_of(c2 * w, w), w)
            ] = both_parts[h * w : (h + 1) * w]

    def finish(c):
        relay(c, other + rest)
        part = lax.dot_general(terms, flipped[c], (((1,), (1,)), ((), ())), preferred_element_type=jnp.float32)
        total = jnp.sum(part, axis=0, keepdims=True) * obs_total ** (-0.5)
        for h in range(2):
            rhs[pl.ds(h * n + c, 1), :] = total[:, h * w : (h + 1) * w]

        def step(k, carry):
            tile(c, k)
            tile(k, c)
            return carry

        lax.fori_loop(0, c, step, 0)
        tile(c, c)

    def phase4(c):
        whole(REST_X, c, other + rest, xn).wait_recv()
        right_out(c, other + rest)

        @pl.when(outer)
        def _():
            s = x * 4 + rest
            relay(c, s)

        relay(c, other + two)
        half(PAIR_Z, c, other + pair, 1 - hz, mate).wait_recv()
        take(c, other + pair)
        take(c, other + rest)
        pl.when(c > 0)(lambda: finish(c - 1))

    each(phase4)
    finish(n - 1)

    def drain(c):
        whole(OWN_X, c, me, xn).wait_send()
        pl.when(has_up)(lambda: whole(OWN_UP, c, me, up).wait_send())
        pl.when(has_down)(lambda: whole(OWN_DOWN, c, me, down).wait_send())

        @pl.when(inner)
        def _():
            whole(TWO_UP, c, me - 1, up).wait_send()
            whole(TWO_DOWN, c, me + 1, down).wait_send()

        pl.when(z == 1)(lambda: whole(THREE_DOWN, c, me, down).wait_send())
        pl.when(z == 2)(lambda: whole(THREE_UP, c, me, up).wait_send())
        half(PAIR_X, c, me, hz, xn).wait_send()
        whole(TWO_X, c, me, xn).wait_send()
        whole(REST_X, c, me, xn).wait_send()
        half(PAIR_Z, c, me, hz, mate).wait_send()

        def pieces(s, carry):
            @pl.when(is_o)
            def _():
                a, b = right_pair(c, s, rows.at[c, hz, s])
                a.wait_send()
                b.wait_send()

            pl.when(is_q)(lambda: relay_copy(c, s).wait_send())
            return carry

        lax.fori_loop(0, 8, pieces, 0)

    each(drain)
    for k, dev in peers:
        wcopy(k, dev).wait_send()


def gathered(design, observed, arc_counts, arc_weight):
    depth, width = design.shape
    n = CHUNKS
    w = width // (2 * n)
    vmem = pl.BlockSpec(memory_space=pltpu.VMEM)
    smem = pl.BlockSpec(memory_space=pltpu.SMEM)
    dma = pltpu.SemaphoreType.DMA
    gram, rhs = pl.pallas_call(
        kernel,
        out_shape=(
            pltpu.VMEM((width, n * w), jnp.float32) if IN_VMEM else jax.ShapeDtypeStruct((width, n * w), jnp.float32),
            jax.ShapeDtypeStruct((2 * n, w), jnp.float32),
        ),
        in_specs=[vmem, vmem, smem, smem],
        out_specs=(vmem, vmem),
        scratch_shapes=[
            pltpu.VMEM((n, 2, 8, depth, w), jnp.bfloat16),
            pltpu.VMEM((n, 8, depth, w), jnp.bfloat16),
            pltpu.VMEM((n, 2 * w, 8 * depth), jnp.bfloat16),
            pltpu.VMEM((n, 8 * depth, w), jnp.bfloat16),
            pltpu.VMEM((8, depth), jnp.float32),
            pltpu.VMEM((8, 8, depth), jnp.float32),
            pltpu.VMEM((8, depth, 128), jnp.float32),
            pltpu.VMEM((8, depth, 128), jnp.float32),
            dma((11, n)),
            dma((11, n)),
            dma((2, n, 8)),
            dma((n, 8)),
            dma((n, 8)),
            dma((8,)),
            dma((8,)),
        ],
        compiler_params=pltpu.CompilerParams(
            collective_id=0, has_side_effects=True, vmem_limit_bytes=VMEM_LIMIT
        ),
    )(design, observed[None, :], arc_counts, arc_weight)
    return gram, rhs.reshape(width)


IN_VMEM = True
VMEM_LIMIT = 40 * 1024 * 1024


def solution(mesh):
    sizes = (mesh.shape["arcs"], mesh.shape["trow"], mesh.shape["tcol"])

    def local(design, observed, arc_counts, arc_weight):
        fits = sizes == (2, 4, 4) and design.shape[0] == 128 and design.shape[1] % (2 * CHUNKS * 128) == 0
        body = gathered if fits else general
        return body(design, observed, arc_counts, arc_weight)

    return jax.shard_map(
        local,
        mesh=mesh,
        in_specs=(
            P(("arcs", "tcol"), "trow"),
            P(("arcs", "tcol")),
            P(("arcs", "tcol")),
            P(("arcs", "tcol")),
        ),
        out_specs=(P("trow", ("arcs", "tcol")), P("trow")),
        check_vma=False,
    )
```

```python
import functools
import jax
import jax.numpy as jnp
from jax import lax
from jax.experimental import pallas as pl
from jax.experimental.pallas import tpu as pltpu
from jax.sharding import PartitionSpec as P

MESH = pl.DeviceIdType.MESH
CHUNKS = 6


def fold_with(right, piece):
    return lax.dot_general(
        piece, right, (((0,), (0,)), ((), ())), preferred_element_type=jnp.float32
    )


def centre(design, observed, arc_counts, arc_weight):
    row_count, col_width = design.shape
    arc_total = arc_counts.shape[0]
    arc_len = row_count // arc_total
    slot_index = lax.broadcasted_iota(jnp.int32, (arc_total, arc_len), 1)
    valid_mask = (slot_index < arc_counts[:, None]).astype(jnp.float32)
    counts_float = arc_counts.astype(jnp.float32)
    factor = valid_mask * jnp.sqrt(arc_weight)[:, None]
    blocks = design.reshape(arc_total, arc_len, col_width).astype(jnp.float32)
    column_mean = jnp.sum(valid_mask[:, :, None] * blocks, axis=1) / counts_float[:, None]
    centered = (
        (factor[:, :, None] * (blocks - column_mean[:, None, :]))
        .reshape(row_count, col_width)
        .astype(jnp.bfloat16)
    )
    series = observed.reshape(arc_total, arc_len)
    series_mean = jnp.sum(valid_mask * series, axis=1) / counts_float
    weighted = (factor * (series - series_mean[:, None])).reshape(row_count)
    return centered, weighted


def general(design, observed, arc_counts, arc_weight):
    centered, weighted = centre(design, observed, arc_counts, arc_weight)
    row_count = design.shape[0]
    arc_devices = lax.axis_size("arcs")
    tcol_devices = lax.axis_size("tcol")
    obs_total = row_count * arc_devices * tcol_devices
    rhs_part = jnp.dot(weighted, centered.astype(jnp.float32), precision=lax.Precision.HIGHEST)
    rhs = lax.psum(rhs_part, ("arcs", "tcol")) * obs_total ** (-0.5)
    every_coef = lax.all_gather(centered, "trow", axis=1, tiled=True)
    full_width = every_coef.shape[1]
    narrow = full_width // (arc_devices * tcol_devices)
    shaped = every_coef.reshape(row_count, arc_devices * tcol_devices, narrow)
    moved = lax.all_to_all(shaped, ("arcs", "tcol"), split_axis=1, concat_axis=0, tiled=True)
    right = moved.reshape(row_count * arc_devices * tcol_devices, narrow)
    tile = fold_with(right, lax.all_gather(centered, ("arcs", "tcol"), axis=0, tiled=True))
    return (tile * (1.0 / obs_total), rhs)


OWN_X, OWN_UP, OWN_DOWN, TWO_UP, TWO_DOWN, THREE_UP, THREE_DOWN, PAIR_X, TWO_X, REST_X, PAIR_Z = range(11)


def kernel(
    design, series, counts, weights, gram, rhs, rows, right, flipped, ready, wown, wall, share, scale,
    ssem, rsem, osem, qsem, rrsem, wssem, wrsem,
):
    n, _, _, depth, w = rows.shape
    arcs_here = counts.shape[0]
    arc_len = depth // arcs_here
    x, t, z = lax.axis_index("arcs"), lax.axis_index("trow"), lax.axis_index("tcol")
    y, core = t // 2, t % 2
    me = x * 4 + z
    other = (1 - x) * 4
    obs_total = 8 * depth
    hz = z % 2
    pair = z + 1 - 2 * hz
    two = (z + 2) % 4
    rest = 3 - z
    xn = (1 - x, t, z)
    up = (x, t, jnp.minimum(z + 1, 3))
    down = (x, t, jnp.maximum(z - 1, 0))
    mate = (x, t, pair)
    partner = (x, t + 1 - 2 * core, z)
    yn = (x, (1 - y) * 2 + core, z)
    lead = core == z // 2
    home = y == x
    is_o = jnp.logical_and(lead, home)
    is_q = jnp.logical_and(lead, jnp.logical_not(home))
    has_up, has_down = z < 3, z > 0
    inner = jnp.logical_and(has_up, has_down)
    outer = jnp.logical_not(inner)
    low, high = z < 2, z >= 2
    early_kind = jnp.where(outer, TWO_X, REST_X)
    late_kind = jnp.where(outer, REST_X, TWO_X)
    early = other + jnp.where(outer, two, rest)
    late = other + jnp.where(outer, rest, two)

    barrier = pltpu.get_barrier_semaphore()
    peers = []
    for dx in range(2):
        for dz in range(4):
            if dx or dz:
                peers.append((dx * 4 + dz, ((x + dx) % 2, t, (z + dz) % 4)))
    for dev in [p for _, p in peers] + [partner, yn]:
        pl.semaphore_signal(barrier, inc=1, device_id=dev, device_id_type=MESH)

    lane = lax.broadcasted_iota(jnp.int32, (8, depth), 1)
    arc = lane // arc_len
    count = jnp.full((8, depth), 1, jnp.int32)
    weight = jnp.zeros((8, depth), jnp.float32)
    for a in range(arcs_here):
        count = jnp.where(arc == a, counts[a], count)
        weight = jnp.where(arc == a, weights[a], weight)
    valid = (lane - arc * arc_len < count).astype(jnp.float32)
    portion = valid / count.astype(jnp.float32)
    factor = valid * jnp.sqrt(weight)
    line = jnp.broadcast_to(series[...], (8, depth))
    average = jnp.zeros((8, depth), jnp.float32)
    for a in range(arcs_here):
        total = jnp.sum(jnp.where(arc == a, valid * line, 0.0), axis=1, keepdims=True)
        average = jnp.where(arc == a, total / count.astype(jnp.float32), average)
    weighted = factor * (line - average)
    level = lax.broadcasted_iota(jnp.int32, (8, depth), 0)
    wown[...] = jnp.where(level == 0, weighted, jnp.where(level == 1, portion, factor))
    wall[me] = wown[...]
    pl.semaphore_wait(barrier, len(peers) + 2)

    def remote(src, dst, send, recv, dev):
        return pltpu.make_async_remote_copy(
            src_ref=src, dst_ref=dst, send_sem=send, recv_sem=recv, device_id=dev, device_id_type=MESH
        )

    def whole(kind, c, s, dev):
        at = rows.at[c, :, s]
        return remote(at, at, ssem.at[kind, c], rsem.at[kind, c], dev)

    def half(kind, c, s, h, dev):
        at = rows.at[c, h, s]
        return remote(at, at, ssem.at[kind, c], rsem.at[kind, c], dev)

    def mine(c, h):
        return design.at[:, pl.ds(pl.multiple_of((h * n + c) * w, w), w)]

    def own(kind, c, dev):
        for h in range(2):
            remote(mine(c, h), rows.at[c, h, me], ssem.at[kind, c], rsem.at[kind, c], dev).start()

    def right_pair(c, s, src):
        at = right.at[c, s]
        return (
            remote(src, at, osem.at[0, c, s], rrsem.at[c, s], partner),
            remote(src, at, osem.at[1, c, s], rrsem.at[c, s], yn),
        )

    def right_out(c, s):
        @pl.when(is_o)
        def _():
            a, b = right_pair(c, s, rows.at[c, hz, s])
            b.start()
            a.start()

    def relay_copy(c, s):
        at = right.at[c, s]
        return remote(at, at, qsem.at[c, s], rrsem.at[c, s], partner)

    def centre_block(block, s):
        wide = block.astype(jnp.float32).reshape(arcs_here, arc_len, w)
        part = jnp.concatenate([share[s]] * (w // 128), axis=1).reshape(arcs_here, arc_len, w)
        gain = jnp.concatenate([scale[s]] * (w // 128), axis=1).reshape(arcs_here, arc_len, w)
        mean = jnp.sum(part * wide, axis=1, keepdims=True)
        return (gain * (wide - mean)).reshape(depth, w).astype(jnp.bfloat16)

    def take(c, s):
        for h in range(2):
            flipped[c, pl.ds(h * w, w), pl.ds(pl.multiple_of(s * depth, depth), depth)] = centre_block(
                rows[c, h, s], s
            ).T

    def relay(c, s):
        @pl.when(jnp.logical_not(is_o))
        def _():
            d = relay_copy(c, s)
            d.wait_recv()
            pl.when(is_q)(d.start)
            ready[c, pl.ds(pl.multiple_of(s * depth, depth), depth), :] = centre_block(right[c, s], s)

        @pl.when(is_o)
        def _():
            ready[c, pl.ds(pl.multiple_of(s * depth, depth), depth), :] = centre_block(rows[c, hz, s], s)

    def each(body):
        def step(c, carry):
            body(c)
            return carry

        lax.fori_loop(0, n, step, 0)

    def wcopy(k, dev):
        return remote(wown, wall.at[me], wssem.at[k], wrsem.at[k], dev)

    def phase0(c):
        own(OWN_X, c, xn)
        pl.when(has_up)(lambda: own(OWN_UP, c, up))
        pl.when(has_down)(lambda: own(OWN_DOWN, c, down))

        @pl.when(is_o)
        def _():
            a, b = right_pair(c, me, mine(c, hz))
            b.start()
            a.start()

    for k, dev in peers:
        wcopy(k, dev).start()
    each(phase0)

    def copy_own(c):
        for h in range(2):
            rows[c, h, me] = design[:, pl.ds(pl.multiple_of((h * n + c) * w, w), w)]

    each(copy_own)
    for k, dev in peers:
        wcopy(k, dev).wait_recv()

    def spread(s, carry):
        columns = wall[s].T
        share[s] = jnp.broadcast_to(columns[:, 1:2], (depth, 128))
        scale[s] = jnp.broadcast_to(columns[:, 2:3], (depth, 128))
        return carry

    lax.fori_loop(0, 8, spread, 0)
    each(lambda c: take(c, me))

    def phase1(c):
        @pl.when(has_down)
        def _():
            whole(OWN_UP, c, me - 1, up).wait_recv()
            pl.when(has_up)(lambda: whole(TWO_UP, c, me - 1, up).start())

        @pl.when(has_up)
        def _():
            whole(OWN_DOWN, c, me + 1, down).wait_recv()
            pl.when(has_down)(lambda: whole(TWO_DOWN, c, me + 1, down).start())

        half(PAIR_X, c, x * 4 + pair, hz, xn).start()
        pl.when(inner)(lambda: whole(REST_X, c, x * 4 + rest, xn).start())
        right_out(c, x * 4 + pair)
        pl.when(inner)(lambda: right_out(c, x * 4 + rest))
        whole(OWN_X, c, other + z, xn).wait_recv()
        right_out(c, other + z)
        take(c, x * 4 + pair)
        pl.when(inner)(lambda: take(c, x * 4 + rest))
        take(c, other + z)
        relay(c, me)

    each(phase1)

    def phase2(c):
        s = x * 4 + two

        @pl.when(low)
        def _():
            whole(TWO_DOWN, c, s, down).wait_recv()
            pl.when(z == 1)(lambda: whole(THREE_DOWN, c, s, down).start())

        @pl.when(high)
        def _():
            whole(TWO_UP, c, s, up).wait_recv()
            pl.when(z == 2)(lambda: whole(THREE_UP, c, s, up).start())

        whole(TWO_X, c, s, xn).start()
        right_out(c, s)
        half(PAIR_X, c, other + pair, hz, xn).wait_recv()
        right_out(c, other + pair)
        take(c, s)
        relay(c, x * 4 + pair)
        pl.when(inner)(lambda: relay(c, x * 4 + rest))
        relay(c, other + z)

    each(phase2)
    each(lambda c: half(PAIR_Z, c, other + z, hz, mate).start())

    def phase3(c):
        @pl.when(outer)
        def _():
            s = x * 4 + rest
            pl.when(z == 0)(lambda: whole(THREE_DOWN, c, s, down).wait_recv())
            pl.when(z == 3)(lambda: whole(THREE_UP, c, s, up).wait_recv())
            whole(REST_X, c, s, xn).start()
            right_out(c, s)
            take(c, s)

        whole(early_kind, c, early, xn).wait_recv()
        right_out(c, early)
        take(c, early)
        relay(c, x * 4 + two)
        relay(c, other + pair)

    each(phase3)

    wide = jnp.concatenate([jnp.broadcast_to(wall[s][0:1], (8, depth)) for s in range(8)], axis=1)
    hi = wide.astype(jnp.bfloat16).astype(jnp.float32)
    mid = (wide - hi).astype(jnp.bfloat16).astype(jnp.float32)
    low_part = wide - hi - mid
    pick = lax.broadcasted_iota(jnp.int32, wide.shape, 0)
    terms = jnp.where(pick == 0, hi, jnp.where(pick == 1, mid, jnp.where(pick == 2, low_part, 0.0)))
    terms = terms.astype(jnp.bfloat16)

    def tile(c1, c2):
        both_parts = lax.dot_general(
            flipped[c1], ready[c2], (((1,), (0,)), ((), ())), preferred_element_type=jnp.float32
        ) * (1.0 / obs_total)
        for h in range(2):
            gram[
                pl.ds(pl.multiple_of(h * n * w + c1 * w, w), w), pl.ds(pl.multiple_of(c2 * w, w), w)
            ] = both_parts[h * w : (h + 1) * w]

    def finish(c):
        relay(c, late)
        part = lax.dot_general(terms, flipped[c], (((1,), (1,)), ((), ())), preferred_element_type=jnp.float32)
        total = jnp.sum(part, axis=0, keepdims=True) * obs_total ** (-0.5)
        for h in range(2):
            rhs[pl.ds(h * n + c, 1), :] = total[:, h * w : (h + 1) * w]

        def step(k, carry):
            tile(c, k)
            tile(k, c)
            return carry

        lax.fori_loop(0, c, step, 0)
        tile(c, c)

    def phase4(c):
        whole(late_kind, c, late, xn).wait_recv()
        right_out(c, late)

        @pl.when(outer)
        def _():
            s = x * 4 + rest
            relay(c, s)

        relay(c, early)
        half(PAIR_Z, c, other + pair, 1 - hz, mate).wait_recv()
        take(c, other + pair)
        take(c, late)
        pl.when(c > 0)(lambda: finish(c - 1))

    each(phase4)
    finish(n - 1)

    def drain(c):
        whole(OWN_X, c, me, xn).wait_send()
        pl.when(has_up)(lambda: whole(OWN_UP, c, me, up).wait_send())
        pl.when(has_down)(lambda: whole(OWN_DOWN, c, me, down).wait_send())

        @pl.when(inner)
        def _():
            whole(TWO_UP, c, me - 1, up).wait_send()
            whole(TWO_DOWN, c, me + 1, down).wait_send()

        pl.when(z == 1)(lambda: whole(THREE_DOWN, c, me, down).wait_send())
        pl.when(z == 2)(lambda: whole(THREE_UP, c, me, up).wait_send())
        half(PAIR_X, c, me, hz, xn).wait_send()
        whole(TWO_X, c, me, xn).wait_send()
        whole(REST_X, c, me, xn).wait_send()
        half(PAIR_Z, c, me, hz, mate).wait_send()

        def pieces(s, carry):
            @pl.when(is_o)
            def _():
                a, b = right_pair(c, s, rows.at[c, hz, s])
                a.wait_send()
                b.wait_send()

            pl.when(is_q)(lambda: relay_copy(c, s).wait_send())
            return carry

        lax.fori_loop(0, 8, pieces, 0)

    each(drain)
    for k, dev in peers:
        wcopy(k, dev).wait_send()


def gathered(design, observed, arc_counts, arc_weight):
    depth, width = design.shape
    n = CHUNKS
    w = width // (2 * n)
    vmem = pl.BlockSpec(memory_space=pltpu.VMEM)
    smem = pl.BlockSpec(memory_space=pltpu.SMEM)
    dma = pltpu.SemaphoreType.DMA
    gram, rhs = pl.pallas_call(
        kernel,
        out_shape=(
            pltpu.VMEM((width, n * w), jnp.float32) if IN_VMEM else jax.ShapeDtypeStruct((width, n * w), jnp.float32),
            jax.ShapeDtypeStruct((2 * n, w), jnp.float32),
        ),
        in_specs=[vmem, vmem, smem, smem],
        out_specs=(vmem, vmem),
        scratch_shapes=[
            pltpu.VMEM((n, 2, 8, depth, w), jnp.bfloat16),
            pltpu.VMEM((n, 8, depth, w), jnp.bfloat16),
            pltpu.VMEM((n, 2 * w, 8 * depth), jnp.bfloat16),
            pltpu.VMEM((n, 8 * depth, w), jnp.bfloat16),
            pltpu.VMEM((8, depth), jnp.float32),
            pltpu.VMEM((8, 8, depth), jnp.float32),
            pltpu.VMEM((8, depth, 128), jnp.float32),
            pltpu.VMEM((8, depth, 128), jnp.float32),
            dma((11, n)),
            dma((11, n)),
            dma((2, n, 8)),
            dma((n, 8)),
            dma((n, 8)),
            dma((8,)),
            dma((8,)),
        ],
        compiler_params=pltpu.CompilerParams(
            collective_id=0, has_side_effects=True, vmem_limit_bytes=VMEM_LIMIT
        ),
    )(design, observed[None, :], arc_counts, arc_weight)
    return gram, rhs.reshape(width)


IN_VMEM = True
VMEM_LIMIT = 40 * 1024 * 1024


def solution(mesh):
    sizes = (mesh.shape["arcs"], mesh.shape["trow"], mesh.shape["tcol"])

    def local(design, observed, arc_counts, arc_weight):
        fits = sizes == (2, 4, 4) and design.shape[0] == 128 and design.shape[1] % (2 * CHUNKS * 128) == 0
        body = gathered if fits else general
        return body(design, observed, arc_counts, arc_weight)

    return jax.shard_map(
        local,
        mesh=mesh,
        in_specs=(
            P(("arcs", "tcol"), "trow"),
            P(("arcs", "tcol")),
            P(("arcs", "tcol")),
            P(("arcs", "tcol")),
        ),
        out_specs=(P("trow", ("arcs", "tcol")), P("trow")),
        check_vma=False,
    )
```
